32 devices in a mesh: sub: 16 (over z, y, x), agg: 2 (over core).
Axes of the slice: x: 2, y: 2, z: 4, core: 2. Of those that a mesh axis runs over, the one named last changes fastest.
Arguments:
- block_values: float32 [7, 4, 4, 32768], P(None, None, None, ('sub', 'agg'))
- block_cols: int32 [7, 32768], P(None, ('sub', 'agg')), may hold values from 0 to 32767, as said below
- coarse_rhs: float32 [4, 32768], P(None, ('sub', 'agg'))
- guess: float32 [4, 32768], P(None, ('sub', 'agg')), may hold values from -3 to 3
- bound_low: int32 [1], replicated, may hold values from 20 to 26
- bound_high: int32 [1], replicated, may hold values from 32 to 40
Outputs:
- smoothed: float32 [4, 32768], P(None, ('sub', 'agg'))
- residual: float32 [4, 32768], P(None, ('sub', 'agg'))
- residual_rms: float32 [1], replicated
The draws below stay inside these ranges and needn't reach their ends.
Inputs may be any that keep to these rules, and one draw needn't show every extreme that they name: Block rows form 32768 / 1024 planes of 1024 consecutive rows, in a periodic order. block_cols[0] is the row itself, block_cols[1] a row of the previous plane, block_cols[2] a row of the next plane, block_cols[3] to block_cols[6] rows of the same plane.
All inputs are finite; a program needn't handle non-finite values.
Results may differ from the reference program's by a relative error of at most 0.0001.
Values sent between devices are 32-bit elements; how exact they have to be, the bound alone decides.
No kernel may reach another device: no remote copies, remote signals or barrier semaphores. Data moves between devices by JAX's collectives and lax.ppermute only.
A program may use at most 64 MiB of HBM per device.

```python
import jax
import jax.numpy as jnp
from jax import lax

ROWS_DEV = 1024
COMP = 4
NEIGHBORS = 7
STEPS = 4
TOTAL = 32768


def draw_block_values(key, part):
    noise = 0.5 * jax.random.normal(key, (NEIGHBORS, COMP, COMP, TOTAL), jnp.float32)
    identity = jnp.eye(COMP, dtype=jnp.float32)[:, :, None]
    diagonal_block = noise[0] * (1.0 - identity) + 6.0 * identity
    return jnp.concatenate([diagonal_block[None], noise[1:]], axis=0)


def draw_block_cols(key, part):
    planes = TOTAL // ROWS_DEV
    rows_all = jnp.arange(TOTAL, dtype=jnp.int32)
    plane_of = rows_all // ROWS_DEV
    picked = jax.random.randint(key, (6, TOTAL), 0, ROWS_DEV).astype(jnp.int32)
    before = (plane_of - 1) % planes * ROWS_DEV + picked[0]
    after = (plane_of + 1) % planes * ROWS_DEV + picked[1]
    same_plane = plane_of[None, :] * ROWS_DEV + picked[2:]
    return jnp.concatenate([rows_all[None], before[None], after[None], same_plane], axis=0).astype(jnp.int32)


def draw_coarse_rhs(key, part):
    rows_all = jnp.arange(TOTAL, dtype=jnp.float32)
    scale_row = 0.5 + 0.5 * rows_all / TOTAL
    values = jax.random.normal(key, (COMP, TOTAL), jnp.float32)
    return values * scale_row[None, :]


def steps_of(own_key, extent, cuts, least, high):
    loudness = 1.0
    for dim, shards_of in cuts:
        draws = jax.random.uniform(jax.random.fold_in(jax.random.fold_in(own_key, 6), dim), (shards_of,), jnp.float32, least / len(cuts), high / len(cuts))
        loudness = loudness * jnp.repeat(jnp.exp(draws), extent[dim] // shards_of).reshape((-1,) + (1,) * (len(extent) - 1 - dim))
    return loudness


def scatter_about(rng, shape, scale, limit, cuts=(), held_as=jnp.bfloat16):
    array = jax.random.normal(rng, shape, jnp.float32) * scale
    if len(cuts) > 0:
        array = steps_of(rng, shape, cuts, -0.22, 0.18) * array
    return jnp.clip(array, min=-limit, max=limit).astype(held_as)


def setup_inputs(seed: int = 0) -> dict:
    splits = jax.random.split(jax.random.key(seed), 7)
    block_values = draw_block_values(jax.random.fold_in(splits[6], 71), 0)
    block_cols = draw_block_cols(jax.random.fold_in(splits[6], 71), 0)
    coarse_rhs = draw_coarse_rhs(jax.random.fold_in(splits[6], 71), 0)
    guess = scatter_about(splits[3], (COMP, TOTAL), 0.5, 3.0, ((1, 32),), jnp.float32)
    bound_low = jax.random.randint(splits[4], (1,), 20, 27).astype(jnp.int32)
    bound_high = jax.random.randint(splits[5], (1,), 32, 41).astype(jnp.int32)
    return dict(block_values=block_values, block_cols=block_cols, coarse_rhs=coarse_rhs, guess=guess, bound_low=bound_low, bound_high=bound_high)


def apply_blocks(block_values, position, field):
    count = position.shape[0]
    width = position.shape[1]
    taken = jnp.take(field, position.reshape(-1), axis=1).reshape(field.shape[0], count, width)
    result = jnp.zeros((field.shape[0], width), jnp.float32)
    for column in range(field.shape[0]):
        result = result + lax.optimization_barrier(jnp.sum(block_values[:, :, column, :] * taken[column][:, None, :], axis=0))
    return result

def reference(block_values, block_cols, coarse_rhs, guess, bound_low, bound_high):
    lower = bound_low[0].astype(jnp.float32) / 4.0
    upper = bound_high[0].astype(jnp.float32) / 4.0
    centre = (upper + lower) / 2.0
    half_width = (upper - lower) / 2.0
    spread_ratio = centre / half_width
    ratio_prev = 1.0 / spread_ratio
    smoothed = guess
    residual = coarse_rhs - apply_blocks(block_values, block_cols, guess)
    direction = residual / centre
    for step in range(STEPS):
        smoothed = smoothed + direction
        residual = residual - apply_blocks(block_values, block_cols, direction)
        if step + 1 < STEPS:
            ratio_next = 1.0 / (2.0 * spread_ratio - ratio_prev)
            direction = ratio_next * ratio_prev * direction + 2.0 * ratio_next / half_width * residual
            ratio_prev = ratio_next
    total_sq = jnp.sum(residual * residual)
    residual_rms = jnp.sqrt(total_sq / (4.0 * TOTAL) + 1e-06).reshape(1)
    return (smoothed, residual, residual_rms)
```

```python
import jax
import jax.numpy as jnp
from jax import lax
from jax.experimental import pallas as pl
from jax.experimental.pallas import tpu as pltpu
from jax.sharding import PartitionSpec as P

STEPS = 4
LANES = 128
AXES = ("sub", "agg")


def shifted(shard, by):
    devices = lax.axis_size(AXES)
    return lax.ppermute(shard, AXES, [(i, (i + by) % devices) for i in range(devices)])


def to_rows(field):
    comp, rows = field.shape[-2:]
    return field.reshape(-1, comp, rows // LANES, LANES).transpose(0, 2, 1, 3).reshape(-1, LANES)


def from_rows(field, comp):
    return field.reshape(-1, comp, LANES).transpose(1, 0, 2).reshape(comp, -1)


def component(ref, c, comp):
    return ref[pl.ds(c, ref.shape[0] // comp, stride=comp), :]


def split_index(cols_ref, k):
    picked = cols_ref[:, k, :]
    chunks = cols_ref.shape[0]
    return picked % LANES, (picked // LANES) % chunks


def gather(source_ref, indices, comp):
    chunks = source_ref.shape[0] // comp
    lanes = [i[0] for i in indices]
    found = [[None] * comp for _ in indices]
    for j in range(chunks):
        masks = [i[1] == j for i in indices]
        for c in range(comp):
            row = jnp.broadcast_to(source_ref[j * comp + c : j * comp + c + 1, :], (chunks, LANES))
            for n, lane in enumerate(lanes):
                taken = jnp.take_along_axis(row, lane, axis=1, mode="promise_in_bounds")
                found[n][c] = taken if j == 0 else jnp.where(masks[n], taken, found[n][c])
    return found


def add_blocks(result, values_ref, k, taken, comp):
    chunks = taken[0].shape[0]
    for a in range(comp):
        for b in range(comp):
            base = ((k * comp + a) * chunks) * comp + b
            block = values_ref[pl.ds(base, chunks, stride=comp), :]
            result[a] = result[a] + block * taken[b]
    return result


def own_part(values_ref, cols_ref, field_ref, comp, neighbors):
    chunks = field_ref.shape[0] // comp
    result = [jnp.zeros((chunks, LANES), jnp.float32) for _ in range(comp)]
    result = add_blocks(result, values_ref, 0, [component(field_ref, c, comp) for c in range(comp)], comp)
    ks = list(range(3, neighbors))
    found = gather(field_ref, [split_index(cols_ref, k) for k in ks], comp)
    for k, taken in zip(ks, found):
        result = add_blocks(result, values_ref, k, taken, comp)
    return result


def far_part(values_ref, cols_ref, below_ref, above_ref, comp):
    chunks = below_ref.shape[0] // comp
    result = [jnp.zeros((chunks, LANES), jnp.float32) for _ in range(comp)]
    for k, source in ((1, below_ref), (2, above_ref)):
        found = gather(source, [split_index(cols_ref, k)], comp)
        result = add_blocks(result, values_ref, k, found[0], comp)
    return result


def coefficients(low_ref, high_ref, shape):
    low = jnp.full(shape, low_ref[0], jnp.int32).astype(jnp.float32) / 4.0
    high = jnp.full(shape, high_ref[0], jnp.int32).astype(jnp.float32) / 4.0
    centre = (high + low) / 2.0
    half = (high - low) / 2.0
    spread = centre / half
    ratio = 1.0 / spread
    rows = [centre]
    for step in range(STEPS - 1):
        following = 1.0 / (2.0 * spread - ratio)
        rows += [following * ratio, 2.0 * following / half]
        ratio = following
    return rows


def kernel_call(body, out_rows, *args, scalars=0, name=None):
    specs = [pl.BlockSpec(memory_space=pltpu.SMEM)] * scalars
    specs += [pl.BlockSpec(memory_space=pltpu.VMEM)] * (len(args) - scalars)
    return pl.pallas_call(
        body,
        out_shape=[jax.ShapeDtypeStruct((rows, LANES), jnp.float32) for rows in out_rows],
        in_specs=specs,
        out_specs=[pl.BlockSpec(memory_space=pltpu.VMEM)] * len(out_rows),
        name=name,
    )(*args)


def shards(block_values, block_cols, coarse_rhs, guess, bound_low, bound_high):
    neighbors, comp, _, rows_own = block_values.shape
    chunks = rows_own // LANES
    devices = lax.axis_size(AXES)
    total_rows = rows_own * devices
    shape = (chunks, LANES)
    field_rows = comp * chunks
    coef_rows = 2 * STEPS - 1

    values = to_rows(block_values.reshape(-1, comp, rows_own))
    cols = block_cols.reshape(neighbors, chunks, LANES).transpose(1, 0, 2)
    rhs = to_rows(coarse_rhs)
    start = to_rows(guess)

    def put(ref, c, value):
        ref[pl.ds(c, chunks, stride=comp), :] = value

    def coef(ref, n):
        return jnp.broadcast_to(ref[n : n + 1, :], shape)

    def first_own(low_ref, high_ref, values_ref, cols_ref, rhs_ref, field_ref, part_ref, coef_ref):
        for n, row in enumerate(coefficients(low_ref, high_ref, (1, LANES))):
            coef_ref[n : n + 1, :] = row
        product = own_part(values_ref, cols_ref, field_ref, comp, neighbors)
        for c in range(comp):
            put(part_ref, c, component(rhs_ref, c, comp) - product[c])

    def first_far(coef_ref, values_ref, cols_ref, below_ref, above_ref, part_ref, residual_ref, direction_ref):
        product = far_part(values_ref, cols_ref, below_ref, above_ref, comp)
        for c in range(comp):
            residual = component(part_ref, c, comp) - product[c]
            put(residual_ref, c, residual)
            put(direction_ref, c, residual / coef(coef_ref, 0))

    def step_own(values_ref, cols_ref, residual_ref, field_ref, smoothed_ref, part_ref, sum_ref):
        sum_ref[...] = smoothed_ref[...] + field_ref[...]
        product = own_part(values_ref, cols_ref, field_ref, comp, neighbors)
        for c in range(comp):
            put(part_ref, c, component(residual_ref, c, comp) - product[c])

    def step_far(step, coef_ref, values_ref, cols_ref, below_ref, above_ref, part_ref, field_ref, residual_ref, direction_ref):
        product = far_part(values_ref, cols_ref, below_ref, above_ref, comp)
        for c in range(comp):
            residual = component(part_ref, c, comp) - product[c]
            put(residual_ref, c, residual)
            put(
                direction_ref,
                c,
                coef(coef_ref, 2 * step + 1) * component(field_ref, c, comp) + coef(coef_ref, 2 * step + 2) * residual,
            )

    def last_far(values_ref, cols_ref, below_ref, above_ref, part_ref, residual_ref, squares_ref):
        product = far_part(values_ref, cols_ref, below_ref, above_ref, comp)
        squares = jnp.zeros(shape, jnp.float32)
        for c in range(comp):
            residual = component(part_ref, c, comp) - product[c]
            put(residual_ref, c, residual)
            squares = squares + residual * residual
        squares_ref[...] = jnp.broadcast_to(jnp.sum(squares, axis=0, keepdims=True), squares_ref.shape)

    below, above = shifted(start, 1), shifted(start, -1)
    part, coefs = kernel_call(
        first_own, (field_rows, coef_rows), bound_low, bound_high, values, cols, rhs, start, scalars=2, name="first_own"
    )
    residual, direction = kernel_call(
        first_far, (field_rows, field_rows), coefs, values, cols, below, above, part, name="first_far"
    )
    smoothed = start
    for step in range(STEPS):
        below, above = shifted(direction, 1), shifted(direction, -1)
        part, smoothed = kernel_call(
            step_own, (field_rows, field_rows), values, cols, residual, direction, smoothed, name="step_own"
        )
        if step + 1 < STEPS:
            residual, direction = kernel_call(
                lambda *refs, step=step: step_far(step, *refs),
                (field_rows, field_rows),
                coefs,
                values,
                cols,
                below,
                above,
                part,
                direction,
                name="step_far",
            )
        else:
            residual, squares = kernel_call(
                last_far, (field_rows, devices), values, cols, below, above, part, name="last_far"
            )
    squares = lax.all_to_all(squares, AXES, 0, 0, tiled=True)
    residual_rms = jnp.sqrt(jnp.sum(squares) / (comp * total_rows) + 1e-06).reshape(1)
    return from_rows(smoothed, comp), from_rows(residual, comp), residual_rms


def solution(mesh):
    return jax.shard_map(
        shards,
        mesh=mesh,
        in_specs=(P(None, None, None, AXES), P(None, AXES), P(None, AXES), P(None, AXES), P(), P()),
        out_specs=(P(None, AXES), P(None, AXES), P()),
        check_vma=False,
    )
```
